32 devices in a mesh: groups: 2 (over x), freq: 16 (over z, y, core).
Axes of the slice: x: 2, y: 2, z: 4, core: 2. Of those that a mesh axis runs over, the one named last changes fastest.
Arguments:
- traces: bfloat16 [1024, 2048, 32], P('freq', None, 'groups'), parts along dimension 2, may hold values from -6 to 6
- freq_index: int32 [16], replicated, may hold values from 1 to 511
- block_map: int32 [64, 64], replicated, may hold values 0 or 1
- green_rec: bfloat16 [16, 2, 2048, 1536], P('freq', None, None, 'groups'), parts along dimension 3, may hold values from -0.1875 to 0.1875
- green_src: bfloat16 [16, 2, 16, 1536], P('freq', None, None, 'groups'), parts along dimension 3, may hold values from -0.25 to 0.25
Outputs:
- image: float32 [1536], P(('groups', 'freq')), parts along dimension 0
The draws below stay inside these ranges and needn't reach their ends.
There are 2 independent parts, one for each index of `groups`. The reference program is written for one: setup_inputs(seed, part) draws one part's arguments, and reference() takes and returns one part's arrays. A program takes and returns all parts, laid end to end along the dimension named above; an argument that names none is the same for every part. Nothing has to cross between parts.
Inputs may be any that keep to these rules, and one draw needn't show every extreme that they name: `freq_index`: frequency bins; they may repeat. `block_map`: 1 where a receiver block lies in an image tile's aperture.
All inputs are finite; a program needn't handle non-finite values.
Results may differ from the reference program's by a relative error of at most 0.0038.
Values may be sent and summed in bfloat16 or wider, within the bound.
A program may use at most 64 MiB of HBM per device.

```python
import math
import jax
import jax.numpy as jnp
from jax import lax

NT = 1024
R = 2048
RBLK = 64
TILES = 64
P_SIZE = 768
S = 16
FREQS = 16


def place_ends(result, key, low, largest):
    extent = result.shape
    spot = [jax.random.randint(jax.random.fold_in(key, axis), (), 0, extent[axis]) for axis in range(len(extent))]
    result = result.at[tuple(spot)].set(low)
    longest = extent.index(max(extent))
    spot[longest] = (spot[longest] + 1) % extent[longest]
    return result.at[tuple(spot)].set(largest)


def strengthened(entries, stream_key, source, target, shards_of, factor):
    owner, partner = [(jnp.arange(entries.shape[axis_at]) // (entries.shape[axis_at] // shards_of)).reshape([-1 if axis == axis_at else 1 for axis in range(entries.ndim)]) for axis_at in (source, target)]
    chosen = jax.random.permutation(stream_key, shards_of)[partner]
    strong = (owner == chosen) | (owner == (partner + shards_of // 2) % shards_of)
    return jnp.where(strong, factor * entries, entries)


def block_levels(key, shape, split, smallest, top_value):
    def one(position, blocks):
        heights = jax.random.uniform(jax.random.fold_in(jax.random.fold_in(key, 6), position), (blocks,), jnp.float32, smallest / len(split), top_value / len(split))
        return jnp.repeat(jnp.exp(heights), shape[position] // blocks).reshape((-1,) + (1,) * (len(shape) - position - 1))

    gain = one(*split[0])
    for cut in split[1:]:
        gain = gain * one(*cut)
    return gain


def centred(key, dims, width, bound, pieces=(), held_as=jnp.bfloat16):
    array = jax.random.normal(key, dims, jnp.float32) * width
    if len(pieces) > 0:
        array = block_levels(key, dims, pieces, -0.22, 0.18) * array
    return jnp.clip(array, min=-bound, max=bound).astype(held_as)


def gaussian_with(rng, extent, width, most, shards, heavy, kind=jnp.bfloat16):
    entries = width * jax.random.normal(rng, extent, jnp.float32)
    if shards:
        entries = entries * block_levels(rng, extent, shards, -0.22, 0.18)
    return jnp.clip(strengthened(entries, jax.random.fold_in(rng, 3), *heavy), -most, most).astype(kind)


def setup_inputs(seed: int = 0, part: int = 0) -> dict:
    key_of = jax.random.split(jax.random.key(seed), 6)
    part_keys = jax.random.split(jax.random.fold_in(key_of[5], part), 6)
    return {
        "traces": gaussian_with(part_keys[0], (NT, R, S), 1.0, 6.0, ((0, 16),), (0, 1, 16, 2.0)),
        "freq_index": place_ends(jax.random.randint(key_of[1], (FREQS,), 1, NT // 2), jax.random.fold_in(key_of[1], 1), 1, (NT // 2) - 1).astype(jnp.int32),
        "block_map": place_ends((jax.random.randint(key_of[2], (RBLK, TILES), 0, 3) < 1).astype(jnp.int32), jax.random.fold_in(key_of[2], 1), 0, 1),
        "green_rec": gaussian_with(part_keys[3], (FREQS, 2, R, P_SIZE), R ** -0.5, 0.1875, ((0, 16),), (0, 3, 16, 2.0)),
        "green_src": centred(part_keys[4], (FREQS, 2, S, P_SIZE), (2 * S * FREQS) ** -0.5, 0.25, ((0, 16),)),
    }


def dft_table(freq_index, length):
    sample_index = jnp.arange(length, dtype=jnp.int32)
    phases = freq_index[:, None] * sample_index[None, :] % length
    angles = phases.astype(jnp.float32) * jnp.float32(2.0 * math.pi / length)
    stacked = jnp.stack((jnp.cos(angles), -jnp.sin(angles)), axis=1)
    return stacked.reshape(freq_index.shape[0] * 2, length).astype(jnp.bfloat16)

def expand_map(block_map, receivers, points):
    row_span = receivers // block_map.shape[0]
    col_span = points // block_map.shape[1]
    return jnp.repeat(jnp.repeat(block_map, row_span, axis=0), col_span, axis=1).astype(jnp.bfloat16)

def reference(traces, freq_index, block_map, green_rec, green_src):
    cos_table = dft_table(freq_index, NT)
    spectrum = jnp.dot(cos_table, traces.reshape(NT, R * S), preferred_element_type=jnp.float32)
    spectrum = (spectrum * (1.0 / math.sqrt(NT))).astype(jnp.bfloat16).reshape(FREQS, 2, R, S)
    mask_full = expand_map(block_map, R, P_SIZE)

    def per_freq(image_sum, stacked):
        spec_f, rec_f, src_f = stacked
        masked = (rec_f * mask_full[None]).astype(jnp.float32)
        spec_w = spec_f.astype(jnp.float32)
        swapped = jnp.stack((spec_w[1], -spec_w[0]), axis=0)
        blocks = jnp.stack((spec_w, swapped), axis=0)
        back_field = jnp.einsum('crx,ocrs->osx', masked, blocks, precision=lax.Precision.HIGHEST)
        image_sum = image_sum + lax.optimization_barrier(jnp.sum(src_f.astype(jnp.float32) * back_field, axis=(0, 1)))
        return (image_sum, None)
    image, _ = lax.scan(per_freq, jnp.zeros((P_SIZE,), jnp.float32), (spectrum, green_rec, green_src))
    return image
```

```python
import functools
import math

import jax
import jax.numpy as jnp
from jax import lax
from jax.experimental import pallas as pl
from jax.experimental.pallas import tpu as pltpu
from jax.sharding import PartitionSpec as P


def dft_table(freq_index, length):
    sample_index = jnp.arange(length, dtype=jnp.int32)
    phases = freq_index[:, None] * sample_index[None, :] % length
    angles = phases.astype(jnp.float32) * jnp.float32(2.0 * math.pi / length)
    stacked = jnp.stack((jnp.cos(angles), -jnp.sin(angles)), axis=1)
    return stacked.reshape(freq_index.shape[0] * 2, length).astype(jnp.bfloat16)


def expand_map(block_map, receivers, points):
    row_span = receivers // block_map.shape[0]
    col_span = points // block_map.shape[1]
    return jnp.repeat(jnp.repeat(block_map, row_span, axis=0), col_span, axis=1).astype(
        jnp.bfloat16
    )


def transform(cos_table, records, length):
    spectrum = jnp.dot(cos_table, records.reshape(length, -1), preferred_element_type=jnp.float32)
    return (spectrum * (1.0 / math.sqrt(length))).astype(jnp.bfloat16)


def back_project(spectra, masked):
    swapped = jnp.stack((spectra[:, 1], -spectra[:, 0]), axis=1)
    blocks = jnp.stack((spectra, swapped), axis=1)
    return jnp.einsum("fcrx,focrs->fosx", masked, blocks, preferred_element_type=jnp.float32)


def body(traces, freq_index, block_map, green_rec, green_src):
    shards = lax.axis_size("freq")
    length = traces.shape[0] * shards
    receivers = traces.shape[1]
    shots = traces.shape[2]
    freqs = freq_index.shape[0]
    cos_table = dft_table(freq_index, length)
    masked = green_rec * expand_map(block_map, receivers, green_rec.shape[3])[None, None]
    regrouped = lax.all_to_all(traces, "freq", split_axis=2, concat_axis=0, tiled=True)
    spectrum = transform(cos_table, regrouped, length).reshape(freqs, 2, receivers, shots // shards)
    gathered = lax.all_to_all(spectrum, "freq", split_axis=0, concat_axis=3, tiled=True)
    back_field = back_project(gathered, masked)
    partial_image = jnp.sum(green_src.astype(jnp.float32) * back_field, axis=(0, 1, 2))
    return lax.psum_scatter(partial_image, "freq", scatter_dimension=0, tiled=True)


CORES = 2
ROWS = 2
CHUNKS = 4
LANES = 128


def seat(cols, row, core):
    return (cols * ROWS + row) * CORES + core


def remote(src, dst, send_sem, recv_sem, target):
    return pltpu.make_async_remote_copy(
        src_ref=src,
        dst_ref=dst,
        send_sem=send_sem,
        recv_sem=recv_sem,
        device_id={"freq": target},
        device_id_type=pl.DeviceIdType.MESH,
    )


def imaging_kernel(
    shots,
    x_ref,
    fi_ref,
    map_ref,
    green_ref,
    src_ref,
    out_ref,
    x_own,
    x_far,
    table,
    y_send,
    y_own,
    y_recv,
    z_send,
    z_own,
    z_recv,
    green_v,
    src_v,
    map_v,
    mask_v,
    acc,
    i_send,
    i_recv,
    x_sem,
    load_sem,
    far_send,
    far_recv,
    ys_sem,
    yr_sem,
    zs_sem,
    zr_sem,
    is_sem,
    ir_sem,
):
    shards = i_send.shape[0]
    cols = shards // (ROWS * CORES)
    local_rows, half = x_own.shape
    samples = local_rows // shots
    length = samples * shards
    chunks, band, width = y_own.shape
    freqs = fi_ref.shape[0]
    receivers = CORES * half
    points = acc.shape[1]
    block = 2 * shots
    bf16, f32 = jnp.bfloat16, jnp.float32

    me = lax.axis_index("freq")
    core = lax.rem(me, CORES)
    row = lax.rem(me // CORES, ROWS)
    col = me // (CORES * ROWS)
    mate = seat(col, row, 1 - core)
    across = seat(col, 1 - row, core)

    barrier = pltpu.get_barrier_semaphore()
    for step in range(1, shards):
        pl.semaphore_signal(
            barrier,
            inc=1,
            device_id={"freq": lax.rem(me + step, shards)},
            device_id_type=pl.DeviceIdType.MESH,
        )

    def lanes(core_at, k):
        return pl.ds(pl.multiple_of(core_at * half + k * width, LANES), width)

    def x_load(k):
        return pltpu.make_async_copy(
            x_ref.at[:, lanes(core, k)], x_own.at[:, pl.ds(k * width, width)], x_sem.at[k]
        )

    def far_copy(k):
        return remote(
            x_ref.at[:, lanes(1 - core, k)],
            x_far.at[:, pl.ds(k * width, width)],
            far_send.at[k],
            far_recv.at[k],
            mate,
        )

    map_load = pltpu.make_async_copy(map_ref, map_v, load_sem.at[0])
    src_load = pltpu.make_async_copy(src_ref, src_v, load_sem.at[1])
    green_load = pltpu.make_async_copy(green_ref, green_v, load_sem.at[2])
    for k in range(chunks):
        x_load(k).start()
    map_load.start()
    src_load.start()
    green_load.start()

    table_rows = 2 * freqs
    span = CORES * samples
    line = lax.broadcasted_iota(jnp.int32, (table_rows, span), 0)
    column = lax.broadcasted_iota(jnp.int32, (table_rows, span), 1)
    bins = jnp.zeros((table_rows, span), jnp.int32)
    for f in range(freqs):
        place = ((f // CORES) % ROWS * cols + f // (CORES * ROWS)) * CORES + f % CORES
        bins = jnp.where(line // 2 == place, fi_ref[f], bins)
    time = jnp.where(column < samples, me * samples + column, (mate - 1) * samples + column)
    angles = lax.rem(bins * time, length).astype(f32) * f32(2.0 * math.pi / length)
    small = jnp.where(line % 2 == 0, jnp.cos(angles), -jnp.sin(angles)).astype(bf16)
    wide = span * shots
    spread = lax.broadcasted_iota(jnp.int32, (span, wide), 1) // shots == lax.broadcasted_iota(
        jnp.int32, (span, wide), 0
    )
    stretched = jnp.dot(small, jnp.where(spread, 1.0, 0.0).astype(bf16), preferred_element_type=f32)
    same_shot = lax.broadcasted_iota(jnp.int32, (shots, wide), 1) % shots == lax.broadcasted_iota(
        jnp.int32, (shots, wide), 0
    )
    for r in range(table_rows):
        spread_row = jnp.broadcast_to(stretched[r : r + 1, :], (shots, wide))
        table[r * shots : (r + 1) * shots, :] = jnp.where(same_shot, spread_row, 0.0).astype(bf16)

    pl.semaphore_wait(barrier, shards - 1)
    for k in range(chunks):
        far_copy(k).start()

    def partial(side, k):
        rows = pl.ds(pl.multiple_of(side * band, band), band)
        at = pl.ds(k * width, width)
        near = jnp.dot(table[rows, :local_rows], x_own[:, at], preferred_element_type=f32)
        return near + jnp.dot(table[rows, local_rows:], x_far[:, at], preferred_element_type=f32)

    def y_copy(k):
        return remote(y_send.at[k], y_recv.at[k], ys_sem.at[k], yr_sem.at[k], across)

    for k in range(chunks):
        x_load(k).wait()
        far_copy(k).wait_recv()
        y_send[k] = partial(1 - row, k).astype(bf16)
        y_copy(k).start()
    for k in range(chunks):
        y_own[k] = partial(row, k)

    map_load.wait()
    tiles = map_v.shape[1]
    in_tile = lax.broadcasted_iota(jnp.int32, (tiles, points), 1) // (
        points // tiles
    ) == lax.broadcasted_iota(jnp.int32, (tiles, points), 0)
    mask_v[...] = jnp.dot(
        map_v[...].astype(f32).astype(bf16),
        jnp.where(in_tile, 1.0, 0.0).astype(bf16),
        preferred_element_type=f32,
    )
    green_load.wait()
    deep = receivers // map_v.shape[0]

    def mask_block(i, carry):
        seen = jnp.broadcast_to(mask_v[pl.ds(i, 1), :], (deep, points)).astype(bf16)
        for part in range(2):
            at = pl.ds(pl.multiple_of(part * receivers + i * deep, deep), deep)
            green_v[at, :] = green_v[at, :] * seen
        return carry

    lax.fori_loop(0, map_v.shape[0], mask_block, 0)
    acc[...] = jnp.zeros_like(acc)

    def block_rows(col_at, core_at):
        return pl.ds(pl.multiple_of((col_at * CORES + core_at) * block, block), block)

    peers = [(dc, dk) for dc in range(cols) for dk in range(CORES) if dc or dk]

    def z_copy(k, dc, dk):
        to_col = lax.rem(col + dc, cols)
        to_core = lax.rem(core + dk, CORES)
        return remote(
            z_send.at[k, block_rows(to_col, to_core), :],
            z_recv.at[col, :, lanes(core, k)],
            zs_sem.at[k, dc, dk],
            zr_sem.at[k, dc, dk],
            seat(to_col, row, to_core),
        )

    def z_arrival(k, dc, dk):
        from_col = lax.rem(col + cols - dc, cols)
        from_core = lax.rem(core + dk, CORES)
        here = z_recv.at[from_col, :, lanes(from_core, k)]
        return remote(here, here, zs_sem.at[k, dc, dk], zr_sem.at[k, dc, dk], mate)

    def scatter(k):
        y_copy(k).wait_recv()
        y_own[k] = y_own[k] + y_recv[k].astype(f32)
        z_send[k] = y_own[k].astype(bf16)
        for dc, dk in peers:
            z_copy(k, dc, dk).start()
        z_own[k] = y_own[k, block_rows(col, core), :]

    def use(spectrum, core_at, k):
        spectrum = spectrum * f32(1.0 / math.sqrt(length))
        turned = jnp.concatenate((spectrum[shots:], -spectrum[:shots]), axis=0)
        first = pl.ds(pl.multiple_of(core_at * half + k * width, width), width)
        second = pl.ds(pl.multiple_of(receivers + core_at * half + k * width, width), width)
        acc[...] += jnp.dot(
            spectrum.astype(bf16), green_v[first, :], preferred_element_type=f32
        ) + jnp.dot(turned.astype(bf16), green_v[second, :], preferred_element_type=f32)

    def consume(k):
        for dk in range(CORES):
            from_core = lax.rem(core + dk, CORES)
            total = None if dk else z_own[k]
            for dc in range(cols):
                if dc or dk:
                    z_arrival(k, dc, dk).wait_recv()
                    from_col = lax.rem(col + cols - dc, cols)
                    term = z_recv[from_col, :, lanes(from_core, k)].astype(f32)
                    total = term if total is None else total + term
            use(total, from_core, k)

    for k in range(chunks):
        scatter(k)
        if k >= 1:
            consume(k - 1)
    consume(chunks - 1)

    src_load.wait()
    product = src_v[...].astype(f32) * acc[...]
    folded = product[0:8]
    for at in range(8, block, 8):
        folded = folded + product[at : at + 8]
    flat = jnp.broadcast_to(jnp.sum(folded, axis=0, keepdims=True), (8, points))
    each = points // shards
    for d in range(shards):
        i_send[d] = pltpu.roll(flat, (points - d * each) % points, 1)[0:1, :LANES]

    def i_copy(step):
        to = lax.rem(me + step, shards)
        return remote(i_send.at[to], i_recv.at[step], is_sem.at[step], ir_sem.at[step], to)

    for step in range(1, shards):
        i_copy(step).start()
    total = i_send[me]
    for step in range(1, shards):
        i_copy(step).wait_recv()
        total = total + i_recv[step]
    out_ref[...] = total

    for k in range(chunks):
        far_copy(k).wait_send()
        y_copy(k).wait_send()
        for dc, dk in peers:
            z_copy(k, dc, dk).wait_send()
    for step in range(1, shards):
        i_copy(step).wait_send()


def fused_body(traces, freq_index, block_map, green_rec, green_src):
    shards = lax.axis_size("freq")
    samples, receivers, shots = traces.shape
    points = green_rec.shape[3]
    freqs = freq_index.shape[0]
    cols = shards // (ROWS * CORES)
    half = receivers // CORES
    width = half // CHUNKS
    records = jnp.transpose(traces, (0, 2, 1)).reshape(samples * shots, receivers)
    green = green_rec.reshape(2 * receivers, points)
    sources = green_src.reshape(2 * shots, points)
    band = 2 * freqs * shots // ROWS
    block = 2 * shots
    bf16, f32 = jnp.bfloat16, jnp.float32
    dma = pltpu.SemaphoreType.DMA
    anywhere = pl.BlockSpec(memory_space=pl.ANY)
    image = pl.pallas_call(
        functools.partial(imaging_kernel, shots),
        out_shape=jax.ShapeDtypeStruct((1, LANES), f32),
        in_specs=[anywhere, pl.BlockSpec(memory_space=pltpu.SMEM), anywhere, anywhere, anywhere],
        out_specs=pl.BlockSpec(memory_space=pltpu.VMEM),
        scratch_shapes=[
            pltpu.VMEM((samples * shots, half), bf16),
            pltpu.VMEM((samples * shots, half), bf16),
            pltpu.VMEM((2 * freqs * shots, CORES * samples * shots), bf16),
            pltpu.VMEM((CHUNKS, band, width), bf16),
            pltpu.VMEM((CHUNKS, band, width), f32),
            pltpu.VMEM((CHUNKS, band, width), bf16),
            pltpu.VMEM((CHUNKS, band, width), bf16),
            pltpu.VMEM((CHUNKS, block, width), f32),
            pltpu.VMEM((cols, block, receivers), bf16),
            pltpu.VMEM((2 * receivers, points), bf16),
            pltpu.VMEM((block, points), bf16),
            pltpu.VMEM(block_map.shape, jnp.int32),
            pltpu.VMEM((block_map.shape[0], points), f32),
            pltpu.VMEM((block, points), f32),
            pltpu.VMEM((shards, 1, LANES), f32),
            pltpu.VMEM((shards, 1, LANES), f32),
            dma((CHUNKS,)),
            dma((3,)),
            dma((CHUNKS,)),
            dma((CHUNKS,)),
            dma((CHUNKS,)),
            dma((CHUNKS,)),
            dma((CHUNKS, cols, CORES)),
            dma((CHUNKS, cols, CORES)),
            dma((shards,)),
            dma((shards,)),
        ],
        compiler_params=pltpu.CompilerParams(
            collective_id=0, has_side_effects=True, vmem_limit_bytes=48 * 1024 * 1024
        ),
    )(records, freq_index, block_map, green, sources)
    return image[0, : points // shards]


def moves_less(traces, freq_index, green_rec):
    shards = lax.axis_size("freq")
    samples, receivers, shots = traces.shape
    freqs = freq_index.shape[0]
    return (
        2 * freqs <= samples
        and freqs == shards
        and shards % (ROWS * CORES) == 0
        and shots % 16 == 0
        and receivers % (CORES * CHUNKS * LANES) == 0
        and green_rec.shape[3] % LANES == 0
        and green_rec.shape[3] // shards <= LANES
    )


def chosen_body(traces, freq_index, block_map, green_rec, green_src):
    fused = moves_less(traces, freq_index, green_rec)
    return (fused_body if fused else body)(traces, freq_index, block_map, green_rec, green_src)


def solution(mesh):
    in_specs = (
        P("freq", None, "groups"),
        P(),
        P(),
        P("freq", None, None, "groups"),
        P("freq", None, None, "groups"),
    )
    out_specs = P(("groups", "freq"))
    return jax.shard_map(chosen_body, mesh=mesh, in_specs=in_specs, out_specs=out_specs, check_vma=False)
```

```python
import functools
import math

import jax
import jax.numpy as jnp
from jax import lax
from jax.experimental import pallas as pl
from jax.experimental.pallas import tpu as pltpu
from jax.sharding import PartitionSpec as P


def dft_table(freq_index, length):
    sample_index = jnp.arange(length, dtype=jnp.int32)
    phases = freq_index[:, None] * sample_index[None, :] % length
    angles = phases.astype(jnp.float32) * jnp.float32(2.0 * math.pi / length)
    stacked = jnp.stack((jnp.cos(angles), -jnp.sin(angles)), axis=1)
    return stacked.reshape(freq_index.shape[0] * 2, length).astype(jnp.bfloat16)


def expand_map(block_map, receivers, points):
    row_span = receivers // block_map.shape[0]
    col_span = points // block_map.shape[1]
    return jnp.repeat(jnp.repeat(block_map, row_span, axis=0), col_span, axis=1).astype(
        jnp.bfloat16
    )


def transform(cos_table, records, length):
    spectrum = jnp.dot(cos_table, records.reshape(length, -1), preferred_element_type=jnp.float32)
    return (spectrum * (1.0 / math.sqrt(length))).astype(jnp.bfloat16)


def back_project(spectra, masked):
    swapped = jnp.stack((spectra[:, 1], -spectra[:, 0]), axis=1)
    blocks = jnp.stack((spectra, swapped), axis=1)
    return jnp.einsum("fcrx,focrs->fosx", masked, blocks, preferred_element_type=jnp.float32)


def body(traces, freq_index, block_map, green_rec, green_src):
    shards = lax.axis_size("freq")
    length = traces.shape[0] * shards
    receivers = traces.shape[1]
    shots = traces.shape[2]
    freqs = freq_index.shape[0]
    cos_table = dft_table(freq_index, length)
    masked = green_rec * expand_map(block_map, receivers, green_rec.shape[3])[None, None]
    regrouped = lax.all_to_all(traces, "freq", split_axis=2, concat_axis=0, tiled=True)
    spectrum = transform(cos_table, regrouped, length).reshape(freqs, 2, receivers, shots // shards)
    gathered = lax.all_to_all(spectrum, "freq", split_axis=0, concat_axis=3, tiled=True)
    back_field = back_project(gathered, masked)
    partial_image = jnp.sum(green_src.astype(jnp.float32) * back_field, axis=(0, 1, 2))
    return lax.psum_scatter(partial_image, "freq", scatter_dimension=0, tiled=True)


CORES = 2
ROWS = 2
CHUNKS = 4
LAG = 2
LANES = 128


def seat(cols, row, core):
    return (cols * ROWS + row) * CORES + core


def remote(src, dst, send_sem, recv_sem, target):
    return pltpu.make_async_remote_copy(
        src_ref=src,
        dst_ref=dst,
        send_sem=send_sem,
        recv_sem=recv_sem,
        device_id={"freq": target},
        device_id_type=pl.DeviceIdType.MESH,
    )


def imaging_kernel(
    shots,
    x_ref,
    fi_hbm,
    map_ref,
    green_ref,
    src_ref,
    out_ref,
    fi_ref,
    x_all,
    x_far,
    table,
    y_send,
    y_own,
    y_recv,
    z_send,
    z_own,
    z_recv,
    green_v,
    src_v,
    map_v,
    mask_v,
    acc,
    i_send,
    i_recv,
    x_sem,
    load_sem,
    far_send,
    far_recv,
    ys_sem,
    yr_sem,
    zs_sem,
    zr_sem,
    is_sem,
    ir_sem,
):
    shards = i_send.shape[0]
    cols = shards // (ROWS * CORES)
    local_rows, half = x_far.shape
    samples = local_rows // shots
    length = samples * shards
    chunks, band, width = y_own.shape
    freqs = fi_ref.shape[0]
    receivers = CORES * half
    points = acc.shape[1]
    block = 2 * shots
    bf16, f32 = jnp.bfloat16, jnp.float32

    me = lax.axis_index("freq")
    core = lax.rem(me, CORES)
    row = lax.rem(me // CORES, ROWS)
    col = me // (CORES * ROWS)
    mate = seat(col, row, 1 - core)
    across = seat(col, 1 - row, core)

    barrier = pltpu.get_barrier_semaphore()
    for step in range(1, shards):
        pl.semaphore_signal(
            barrier,
            inc=1,
            device_id={"freq": lax.rem(me + step, shards)},
            device_id_type=pl.DeviceIdType.MESH,
        )

    def lanes(core_at, k):
        return pl.ds(pl.multiple_of(core_at * half + k * width, LANES), width)

    def x_load(core_at):
        side = pl.ds(pl.multiple_of(core_at * half, LANES), half)
        return pltpu.make_async_copy(x_ref.at[:, side], x_all.at[:, side], x_sem.at[core_at])

    def far_copy(k):
        return remote(
            x_all.at[:, lanes(1 - core, k)],
            x_far.at[:, pl.ds(k * width, width)],
            far_send,
            far_recv.at[k],
            mate,
        )

    fi_load = pltpu.make_async_copy(fi_hbm, fi_ref, load_sem.at[3])
    map_load = pltpu.make_async_copy(map_ref, map_v, load_sem.at[0])
    src_load = pltpu.make_async_copy(src_ref, src_v, load_sem.at[1])
    green_load = pltpu.make_async_copy(green_ref, green_v, load_sem.at[2])
    fi_load.start()
    x_load(1 - core).start()
    x_load(core).start()
    map_load.start()
    src_load.start()
    green_load.start()

    table_rows = 2 * freqs
    span = CORES * samples
    line = lax.broadcasted_iota(jnp.int32, (table_rows, span), 0)
    column = lax.broadcasted_iota(jnp.int32, (table_rows, span), 1)
    fi_load.wait()
    bins = jnp.zeros((table_rows, span), jnp.int32)
    for f in range(freqs):
        place = ((f // CORES) % ROWS * cols + f // (CORES * ROWS)) * CORES + f % CORES
        bins = jnp.where(line // 2 == place, fi_ref[f], bins)
    time = jnp.where(column < samples, me * samples + column, (mate - 1) * samples + column)
    angles = lax.rem(bins * time, length).astype(f32) * f32(2.0 * math.pi / length)
    small = jnp.where(line % 2 == 0, jnp.cos(angles), -jnp.sin(angles)).astype(bf16)
    wide = span * shots
    spread = lax.broadcasted_iota(jnp.int32, (span, wide), 1) // shots == lax.broadcasted_iota(
        jnp.int32, (span, wide), 0
    )
    stretched = jnp.dot(small, jnp.where(spread, 1.0, 0.0).astype(bf16), preferred_element_type=f32)
    same_shot = lax.broadcasted_iota(jnp.int32, (shots, wide), 1) % shots == lax.broadcasted_iota(
        jnp.int32, (shots, wide), 0
    )
    for r in range(table_rows):
        spread_row = jnp.broadcast_to(stretched[r : r + 1, :], (shots, wide))
        table[r * shots : (r + 1) * shots, :] = jnp.where(same_shot, spread_row, 0.0).astype(bf16)

    pl.semaphore_wait(barrier, shards - 1)
    x_load(1 - core).wait()
    for k in range(chunks):
        far_copy(k).start()

    def partial(side, k):
        rows = pl.ds(pl.multiple_of(side * band, band), band)
        at = pl.ds(k * width, width)
        near = jnp.dot(table[rows, :local_rows], x_all[:, lanes(core, k)], preferred_element_type=f32)
        return near + jnp.dot(table[rows, local_rows:], x_far[:, at], preferred_element_type=f32)

    def y_copy(k):
        return remote(y_send.at[k], y_recv.at[k], ys_sem, yr_sem.at[k], across)

    x_load(core).wait()
    for k in range(chunks):
        far_copy(k).wait_recv()
        y_send[k] = partial(1 - row, k).astype(bf16)
        y_copy(k).start()
    for k in range(chunks):
        y_own[k] = partial(row, k)

    map_load.wait()
    tiles = map_v.shape[1]
    in_tile = lax.broadcasted_iota(jnp.int32, (tiles, points), 1) // (
        points // tiles
    ) == lax.broadcasted_iota(jnp.int32, (tiles, points), 0)
    mask_v[...] = jnp.dot(
        map_v[...].astype(f32).astype(bf16),
        jnp.where(in_tile, 1.0, 0.0).astype(bf16),
        preferred_element_type=f32,
    )
    green_load.wait()
    deep = receivers // map_v.shape[0]

    def mask_block(i, carry):
        seen = jnp.broadcast_to(mask_v[pl.ds(i, 1), :], (deep, points)).astype(bf16)
        for part in range(2):
            at = pl.ds(pl.multiple_of(part * receivers + i * deep, deep), deep)
            green_v[at, :] = green_v[at, :] * seen
        return carry

    lax.fori_loop(0, map_v.shape[0], mask_block, 0)
    acc[...] = jnp.zeros_like(acc)

    def block_rows(col_at, core_at):
        return pl.ds(pl.multiple_of((col_at * CORES + core_at) * block, block), block)

    peers = [(dc, dk) for dc in range(cols) for dk in range(CORES) if dc or dk]

    def z_copy(k, dc, dk):
        to_col = lax.rem(col + dc, cols)
        to_core = lax.rem(core + dk, CORES)
        return remote(
            z_send.at[k, block_rows(to_col, to_core), :],
            z_recv.at[col, :, lanes(core, k)],
            zs_sem,
            zr_sem.at[k],
            seat(to_col, row, to_core),
        )

    def z_arrival(k):
        every = z_send.at[k, pl.ds(0, len(peers) * block), :]
        return pltpu.make_async_copy(every, every, zr_sem.at[k])

    def scatter(k):
        y_copy(k).wait_recv()
        y_own[k] = y_own[k] + y_recv[k].astype(f32)
        z_send[k] = y_own[k].astype(bf16)
        for dc, dk in peers:
            z_copy(k, dc, dk).start()
        z_own[k] = y_own[k, block_rows(col, core), :]

    def use(spectrum, core_at, k):
        spectrum = spectrum * f32(1.0 / math.sqrt(length))
        turned = jnp.concatenate((spectrum[shots:], -spectrum[:shots]), axis=0)
        first = pl.ds(pl.multiple_of(core_at * half + k * width, width), width)
        second = pl.ds(pl.multiple_of(receivers + core_at * half + k * width, width), width)
        acc[...] += jnp.dot(
            spectrum.astype(bf16), green_v[first, :], preferred_element_type=f32
        ) + jnp.dot(turned.astype(bf16), green_v[second, :], preferred_element_type=f32)

    def consume(k):
        z_arrival(k).wait()
        for dk in range(CORES):
            from_core = lax.rem(core + dk, CORES)
            total = None if dk else z_own[k]
            for dc in range(cols):
                if dc or dk:
                    from_col = lax.rem(col + cols - dc, cols)
                    term = z_recv[from_col, :, lanes(from_core, k)].astype(f32)
                    total = term if total is None else total + term
            use(total, from_core, k)

    for k in range(chunks):
        scatter(k)
        if k >= LAG:
            consume(k - LAG)
    for k in range(chunks - LAG, chunks):
        consume(k)

    src_load.wait()
    product = src_v[...].astype(f32) * acc[...]
    folded = product[0:8]
    for at in range(8, block, 8):
        folded = folded + product[at : at + 8]
    flat = jnp.broadcast_to(jnp.sum(folded, axis=0, keepdims=True), (8, points))
    each = points // shards
    for d in range(shards):
        i_send[d] = pltpu.roll(flat, (points - d * each) % points, 1)[0:1, :LANES]

    def i_copy(step):
        to = lax.rem(me + step, shards)
        return remote(i_send.at[to], i_recv.at[step], is_sem, ir_sem, to)

    for step in range(1, shards):
        i_copy(step).start()
    total = i_send[me]
    others = i_recv.at[pl.ds(1, shards - 1)]
    pltpu.make_async_copy(others, others, ir_sem).wait()
    for step in range(1, shards):
        total = total + i_recv[step]
    out_ref[...] = total

    z_sent = z_send.at[:, pl.ds(0, len(peers) * block), :]
    for sent, sem in ((x_far, far_send), (y_send, ys_sem), (z_sent, zs_sem), (others, is_sem)):
        pltpu.make_async_copy(sent, sent, sem).wait()


def fused_body(traces, freq_index, block_map, green_rec, green_src):
    shards = lax.axis_size("freq")
    samples, receivers, shots = traces.shape
    points = green_rec.shape[3]
    freqs = freq_index.shape[0]
    cols = shards // (ROWS * CORES)
    half = receivers // CORES
    width = half // CHUNKS
    records = jnp.transpose(traces, (0, 2, 1)).reshape(samples * shots, receivers)
    green = green_rec.reshape(2 * receivers, points)
    sources = green_src.reshape(2 * shots, points)
    band = 2 * freqs * shots // ROWS
    block = 2 * shots
    bf16, f32 = jnp.bfloat16, jnp.float32
    dma = pltpu.SemaphoreType.DMA
    outside = pl.BlockSpec(memory_space=pltpu.HBM)
    image = pl.pallas_call(
        functools.partial(imaging_kernel, shots),
        out_shape=jax.ShapeDtypeStruct((1, LANES), f32),
        in_specs=[outside] * 5,
        out_specs=pl.BlockSpec(memory_space=pltpu.VMEM),
        scratch_shapes=[
            pltpu.SMEM(freq_index.shape, jnp.int32),
            pltpu.VMEM((samples * shots, receivers), bf16),
            pltpu.VMEM((samples * shots, half), bf16),
            pltpu.VMEM((2 * freqs * shots, CORES * samples * shots), bf16),
            pltpu.VMEM((CHUNKS, band, width), bf16),
            pltpu.VMEM((CHUNKS, band, width), f32),
            pltpu.VMEM((CHUNKS, band, width), bf16),
            pltpu.VMEM((CHUNKS, band, width), bf16),
            pltpu.VMEM((CHUNKS, block, width), f32),
            pltpu.VMEM((cols, block, receivers), bf16),
            pltpu.VMEM((2 * receivers, points), bf16),
            pltpu.VMEM((block, points), bf16),
            pltpu.VMEM(block_map.shape, jnp.int32),
            pltpu.VMEM((block_map.shape[0], points), f32),
            pltpu.VMEM((block, points), f32),
            pltpu.VMEM((shards, 1, LANES), f32),
            pltpu.VMEM((shards, 1, LANES), f32),
            dma((CORES,)),
            dma((4,)),
            dma,
            dma((CHUNKS,)),
            dma,
            dma((CHUNKS,)),
            dma,
            dma((CHUNKS,)),
            dma,
            dma,
        ],
        compiler_params=pltpu.CompilerParams(
            collective_id=0, has_side_effects=True, vmem_limit_bytes=48 * 1024 * 1024
        ),
    )(
        *(
            pltpu.with_memory_space_constraint(array, pltpu.HBM)
            for array in (records, freq_index, block_map, green, sources)
        )
    )
    return image[0, : points // shards]


def moves_less(traces, freq_index, green_rec):
    shards = lax.axis_size("freq")
    samples, receivers, shots = traces.shape
    freqs = freq_index.shape[0]
    return (
        2 * freqs <= samples
        and freqs == shards
        and shards % (ROWS * CORES) == 0
        and shots % 16 == 0
        and receivers % (CORES * CHUNKS * LANES) == 0
        and green_rec.shape[3] % LANES == 0
        and green_rec.shape[3] // shards <= LANES
    )


def chosen_body(traces, freq_index, block_map, green_rec, green_src):
    fused = moves_less(traces, freq_index, green_rec)
    return (fused_body if fused else body)(traces, freq_index, block_map, green_rec, green_src)


def solution(mesh):
    in_specs = (
        P("freq", None, "groups"),
        P(),
        P(),
        P("freq", None, None, "groups"),
        P("freq", None, None, "groups"),
    )
    out_specs = P(("groups", "freq"))
    return jax.shard_map(chosen_body, mesh=mesh, in_specs=in_specs, out_specs=out_specs, check_vma=False)
```

```python
import functools
import math

import jax
import jax.numpy as jnp
from jax import lax
from jax.experimental import pallas as pl
from jax.experimental.pallas import tpu as pltpu
from jax.sharding import PartitionSpec as P


def dft_table(freq_index, length):
    sample_index = jnp.arange(length, dtype=jnp.int32)
    phases = freq_index[:, None] * sample_index[None, :] % length
    angles = phases.astype(jnp.float32) * jnp.float32(2.0 * math.pi / length)
    stacked = jnp.stack((jnp.cos(angles), -jnp.sin(angles)), axis=1)
    return stacked.reshape(freq_index.shape[0] * 2, length).astype(jnp.bfloat16)


def expand_map(block_map, receivers, points):
    row_span = receivers // block_map.shape[0]
    col_span = points // block_map.shape[1]
    return jnp.repeat(jnp.repeat(block_map, row_span, axis=0), col_span, axis=1).astype(
        jnp.bfloat16
    )


def transform(cos_table, records, length):
    spectrum = jnp.dot(cos_table, records.reshape(length, -1), preferred_element_type=jnp.float32)
    return (spectrum * (1.0 / math.sqrt(length))).astype(jnp.bfloat16)


def back_project(spectra, masked):
    swapped = jnp.stack((spectra[:, 1], -spectra[:, 0]), axis=1)
    blocks = jnp.stack((spectra, swapped), axis=1)
    return jnp.einsum("fcrx,focrs->fosx", masked, blocks, preferred_element_type=jnp.float32)


def body(traces, freq_index, block_map, green_rec, green_src):
    shards = lax.axis_size("freq")
    length = traces.shape[0] * shards
    receivers = traces.shape[1]
    shots = traces.shape[2]
    freqs = freq_index.shape[0]
    cos_table = dft_table(freq_index, length)
    masked = green_rec * expand_map(block_map, receivers, green_rec.shape[3])[None, None]
    regrouped = lax.all_to_all(traces, "freq", split_axis=2, concat_axis=0, tiled=True)
    spectrum = transform(cos_table, regrouped, length).reshape(freqs, 2, receivers, shots // shards)
    gathered = lax.all_to_all(spectrum, "freq", split_axis=0, concat_axis=3, tiled=True)
    back_field = back_project(gathered, masked)
    partial_image = jnp.sum(green_src.astype(jnp.float32) * back_field, axis=(0, 1, 2))
    return lax.psum_scatter(partial_image, "freq", scatter_dimension=0, tiled=True)


CORES = 2
ROWS = 2
LAG = 4
LANES = 128


def bands(half):
    return tuple((start, LANES) for start in range(0, half, LANES))


def seat(cols, row, core):
    return (cols * ROWS + row) * CORES + core


def remote(src, dst, send_sem, recv_sem, target):
    return pltpu.make_async_remote_copy(
        src_ref=src,
        dst_ref=dst,
        send_sem=send_sem,
        recv_sem=recv_sem,
        device_id={"freq": target},
        device_id_type=pl.DeviceIdType.MESH,
    )


def imaging_kernel(
    shots,
    x_ref,
    fi_hbm,
    map_ref,
    green_ref,
    src_ref,
    out_ref,
    fi_ref,
    x_all,
    x_far,
    table,
    y_send,
    y_own,
    y_recv,
    z_send,
    z_own,
    z_recv,
    green_v,
    src_v,
    map_v,
    mask_v,
    acc,
    i_send,
    i_recv,
    x_sem,
    load_sem,
    far_send,
    far_recv,
    ys_sem,
    yr_sem,
    zs_sem,
    zr_sem,
    is_sem,
    ir_sem,
):
    shards = i_send.shape[0]
    cols = shards // (ROWS * CORES)
    local_rows, half = x_far.shape
    samples = local_rows // shots
    length = samples * shards
    band = y_own.shape[0]
    steps = bands(half)
    chunks = len(steps)
    freqs = fi_ref.shape[0]
    receivers = CORES * half
    points = acc.shape[1]
    block = 2 * shots
    bf16, f32 = jnp.bfloat16, jnp.float32

    me = lax.axis_index("freq")
    core = lax.rem(me, CORES)
    row = lax.rem(me // CORES, ROWS)
    col = me // (CORES * ROWS)
    mate = seat(col, row, 1 - core)
    across = seat(col, 1 - row, core)

    barrier = pltpu.get_barrier_semaphore()
    for step in range(1, shards):
        pl.semaphore_signal(
            barrier,
            inc=1,
            device_id={"freq": lax.rem(me + step, shards)},
            device_id_type=pl.DeviceIdType.MESH,
        )

    def lanes(core_at, k):
        return pl.ds(pl.multiple_of(core_at * half + steps[k][0], LANES), steps[k][1])

    def x_load(core_at):
        side = pl.ds(pl.multiple_of(core_at * half, LANES), half)
        return pltpu.make_async_copy(x_ref.at[:, side], x_all.at[:, side], x_sem.at[core_at])

    def far_copy(k):
        return remote(
            x_all.at[:, lanes(1 - core, k)],
            x_far.at[:, pl.ds(*steps[k])],
            far_send,
            far_recv.at[k],
            mate,
        )

    fi_load = pltpu.make_async_copy(fi_hbm, fi_ref, load_sem.at[3])
    map_load = pltpu.make_async_copy(map_ref, map_v, load_sem.at[0])
    src_load = pltpu.make_async_copy(src_ref, src_v, load_sem.at[1])
    green_load = pltpu.make_async_copy(green_ref, green_v, load_sem.at[2])
    fi_load.start()
    x_load(1 - core).start()
    x_load(core).start()
    map_load.start()
    src_load.start()
    green_load.start()

    table_rows = 2 * freqs
    span = CORES * samples
    line = lax.broadcasted_iota(jnp.int32, (table_rows, span), 0)
    column = lax.broadcasted_iota(jnp.int32, (table_rows, span), 1)
    fi_load.wait()
    bins = jnp.zeros((table_rows, span), jnp.int32)
    for f in range(freqs):
        place = ((f // CORES) % ROWS * cols + f // (CORES * ROWS)) * CORES + f % CORES
        bins = jnp.where(line // 2 == place, fi_ref[f], bins)
    time = jnp.where(column < samples, me * samples + column, (mate - 1) * samples + column)
    angles = lax.rem(bins * time, length).astype(f32) * f32(2.0 * math.pi / length)
    small = jnp.where(line % 2 == 0, jnp.cos(angles), -jnp.sin(angles)).astype(bf16)
    wide = span * shots
    spread = lax.broadcasted_iota(jnp.int32, (span, wide), 1) // shots == lax.broadcasted_iota(
        jnp.int32, (span, wide), 0
    )
    stretched = jnp.dot(small, jnp.where(spread, 1.0, 0.0).astype(bf16), preferred_element_type=f32)
    same_shot = lax.broadcasted_iota(jnp.int32, (shots, wide), 1) % shots == lax.broadcasted_iota(
        jnp.int32, (shots, wide), 0
    )
    for r in range(table_rows):
        spread_row = jnp.broadcast_to(stretched[r : r + 1, :], (shots, wide))
        table[r * shots : (r + 1) * shots, :] = jnp.where(same_shot, spread_row, 0.0).astype(bf16)

    pl.semaphore_wait(barrier, shards - 1)
    x_load(1 - core).wait()
    for k in range(chunks):
        far_copy(k).start()

    def partial(side, k):
        rows = pl.ds(pl.multiple_of(side * band, band), band)
        at = pl.ds(*steps[k])
        near = jnp.dot(table[rows, :local_rows], x_all[:, lanes(core, k)], preferred_element_type=f32)
        return near + jnp.dot(table[rows, local_rows:], x_far[:, at], preferred_element_type=f32)

    def y_copy(k):
        at = pl.ds(*steps[k])
        return remote(y_send.at[:, at], y_recv.at[:, at], ys_sem, yr_sem.at[k], across)

    def send_partial(k):
        far_copy(k).wait_recv()
        y_send[:, pl.ds(*steps[k])] = partial(1 - row, k).astype(bf16)
        y_copy(k).start()

    def keep_partial(k):
        y_own[:, pl.ds(*steps[k])] = partial(row, k)

    def block_rows(col_at, core_at):
        return pl.ds(pl.multiple_of((col_at * CORES + core_at) * block, block), block)

    peers = [(dc, dk) for dc in range(cols) for dk in range(CORES) if dc or dk]

    def z_copy(k, dc, dk):
        to_col = lax.rem(col + dc, cols)
        to_core = lax.rem(core + dk, CORES)
        return remote(
            z_send.at[block_rows(to_col, to_core), pl.ds(*steps[k])],
            z_recv.at[col, :, lanes(core, k)],
            zs_sem,
            zr_sem.at[k],
            seat(to_col, row, to_core),
        )

    def scatter(k):
        y_copy(k).wait_recv()
        at = pl.ds(*steps[k])
        y_own[:, at] = y_own[:, at] + y_recv[:, at].astype(f32)
        z_send[:, at] = y_own[:, at].astype(bf16)
        for dc, dk in peers:
            z_copy(k, dc, dk).start()
        z_own[:, at] = y_own[block_rows(col, core), at]
    x_load(core).wait()
    for k in range(chunks):
        send_partial(k)
        if k % 4 == 3:
            keep_partial(k // 4)
    early = (chunks + 3) // 4
    for k in range(chunks // 4, early):
        keep_partial(k)
    scatter(0)
    keep_partial(early)
    scatter(1)
    for k in range(early + 1, min(early + 2, chunks)):
        keep_partial(k)

    map_load.wait()
    tiles = map_v.shape[1]
    in_tile = lax.broadcasted_iota(jnp.int32, (tiles, points), 1) // (
        points // tiles
    ) == lax.broadcasted_iota(jnp.int32, (tiles, points), 0)
    mask_v[...] = jnp.dot(
        map_v[...].astype(f32).astype(bf16),
        jnp.where(in_tile, 1.0, 0.0).astype(bf16),
        preferred_element_type=f32,
    )
    green_load.wait()
    deep = receivers // map_v.shape[0]

    def mask_block(i, carry):
        seen = jnp.broadcast_to(mask_v[pl.ds(i, 1), :], (deep, points)).astype(bf16)
        for part in range(2):
            at = pl.ds(pl.multiple_of(part * receivers + i * deep, deep), deep)
            green_v[at, :] = green_v[at, :] * seen
        return carry

    lax.fori_loop(0, map_v.shape[0], mask_block, 0)
    acc[...] = jnp.zeros_like(acc)

    def z_arrival(k):
        every = z_send.at[pl.ds(0, len(peers) * block), pl.ds(*steps[k])]
        return pltpu.make_async_copy(every, every, zr_sem.at[k])

    def use(spectrum, core_at, k):
        spectrum = spectrum * f32(1.0 / math.sqrt(length))
        turned = jnp.concatenate((spectrum[shots:], -spectrum[:shots]), axis=0)
        first = lanes(core_at, k)
        second = lanes(CORES + core_at, k)
        acc[...] += jnp.dot(
            spectrum.astype(bf16), green_v[first, :], preferred_element_type=f32
        ) + jnp.dot(turned.astype(bf16), green_v[second, :], preferred_element_type=f32)

    def consume(k):
        z_arrival(k).wait()
        for dk in range(CORES):
            from_core = lax.rem(core + dk, CORES)
            total = None if dk else z_own[:, pl.ds(*steps[k])]
            for dc in range(cols):
                if dc or dk:
                    from_col = lax.rem(col + cols - dc, cols)
                    term = z_recv[from_col, :, lanes(from_core, k)].astype(f32)
                    total = term if total is None else total + term
            use(total, from_core, k)

    for k in range(2, chunks):
        scatter(k)
        for at in range(early + 2 * k - 2, min(early + 2 * k, chunks)):
            keep_partial(at)
        if k >= LAG:
            consume(k - LAG)
    for k in range(chunks - LAG, chunks):
        consume(k)

    src_load.wait()
    product = src_v[...].astype(f32) * acc[...]
    folded = product[0:8]
    for at in range(8, block, 8):
        folded = folded + product[at : at + 8]
    flat = jnp.broadcast_to(jnp.sum(folded, axis=0, keepdims=True), (8, points))
    each = points // shards
    for d in range(shards):
        i_send[d] = pltpu.roll(flat, (points - d * each) % points, 1)[0:1, :LANES]

    def i_copy(step):
        to = lax.rem(me + step, shards)
        return remote(i_send.at[to], i_recv.at[step], is_sem, ir_sem, to)

    for step in range(1, shards):
        i_copy(step).start()
    total = i_send[me]
    others = i_recv.at[pl.ds(1, shards - 1)]
    pltpu.make_async_copy(others, others, ir_sem).wait()
    for step in range(1, shards):
        total = total + i_recv[step]
    out_ref[...] = total

    z_sent = z_send.at[pl.ds(0, len(peers) * block), :]
    for sent, sem in ((x_far, far_send), (y_send, ys_sem), (z_sent, zs_sem), (others, is_sem)):
        pltpu.make_async_copy(sent, sent, sem).wait()


def fused_body(traces, freq_index, block_map, green_rec, green_src):
    shards = lax.axis_size("freq")
    samples, receivers, shots = traces.shape
    points = green_rec.shape[3]
    freqs = freq_index.shape[0]
    cols = shards // (ROWS * CORES)
    half = receivers // CORES
    chunks = len(bands(half))
    records = jnp.transpose(traces, (0, 2, 1)).reshape(samples * shots, receivers)
    green = green_rec.reshape(2 * receivers, points)
    sources = green_src.reshape(2 * shots, points)
    band = 2 * freqs * shots // ROWS
    block = 2 * shots
    bf16, f32 = jnp.bfloat16, jnp.float32
    dma = pltpu.SemaphoreType.DMA
    outside = pl.BlockSpec(memory_space=pltpu.HBM)
    image = pl.pallas_call(
        functools.partial(imaging_kernel, shots),
        out_shape=jax.ShapeDtypeStruct((1, LANES), f32),
        in_specs=[outside] * 5,
        out_specs=pl.BlockSpec(memory_space=pltpu.VMEM),
        scratch_shapes=[
            pltpu.SMEM(freq_index.shape, jnp.int32),
            pltpu.VMEM((samples * shots, receivers), bf16),
            pltpu.VMEM((samples * shots, half), bf16),
            pltpu.VMEM((2 * freqs * shots, CORES * samples * shots), bf16),
            pltpu.VMEM((band, half), bf16),
            pltpu.VMEM((band, half), f32),
            pltpu.VMEM((band, half), bf16),
            pltpu.VMEM((band, half), bf16),
            pltpu.VMEM((block, half), f32),
            pltpu.VMEM((cols, block, receivers), bf16),
            pltpu.VMEM((2 * receivers, points), bf16),
            pltpu.VMEM((block, points), bf16),
            pltpu.VMEM(block_map.shape, jnp.int32),
            pltpu.VMEM((block_map.shape[0], points), f32),
            pltpu.VMEM((block, points), f32),
            pltpu.VMEM((shards, 1, LANES), f32),
            pltpu.VMEM((shards, 1, LANES), f32),
            dma((CORES,)),
            dma((4,)),
            dma,
            dma((chunks,)),
            dma,
            dma((chunks,)),
            dma,
            dma((chunks,)),
            dma,
            dma,
        ],
        compiler_params=pltpu.CompilerParams(
            collective_id=0, has_side_effects=True, vmem_limit_bytes=48 * 1024 * 1024
        ),
    )(
        *(
            pltpu.with_memory_space_constraint(array, pltpu.HBM)
            for array in (records, freq_index, block_map, green, sources)
        )
    )
    return image[0, : points // shards]


def moves_less(traces, freq_index, green_rec):
    shards = lax.axis_size("freq")
    samples, receivers, shots = traces.shape
    freqs = freq_index.shape[0]
    return (
        2 * freqs <= samples
        and freqs == shards
        and shards % (ROWS * CORES) == 0
        and shots % 16 == 0
        and receivers % (CORES * 4 * LANES) == 0
        and green_rec.shape[3] % LANES == 0
        and green_rec.shape[3] // shards <= LANES
    )


def chosen_body(traces, freq_index, block_map, green_rec, green_src):
    fused = moves_less(traces, freq_index, green_rec)
    return (fused_body if fused else body)(traces, freq_index, block_map, green_rec, green_src)


def solution(mesh):
    in_specs = (
        P("freq", None, "groups"),
        P(),
        P(),
        P("freq", None, None, "groups"),
        P("freq", None, None, "groups"),
    )
    out_specs = P(("groups", "freq"))
    return jax.shard_map(chosen_body, mesh=mesh, in_specs=in_specs, out_specs=out_specs, check_vma=False)
```

```python
import functools
import math

import jax
import jax.numpy as jnp
from jax import lax
from jax.experimental import pallas as pl
from jax.experimental.pallas import tpu as pltpu
from jax.sharding import PartitionSpec as P


def dft_table(freq_index, length):
    sample_index = jnp.arange(length, dtype=jnp.int32)
    phases = freq_index[:, None] * sample_index[None, :] % length
    angles = phases.astype(jnp.float32) * jnp.float32(2.0 * math.pi / length)
    stacked = jnp.stack((jnp.cos(angles), -jnp.sin(angles)), axis=1)
    return stacked.reshape(freq_index.shape[0] * 2, length).astype(jnp.bfloat16)


def expand_map(block_map, receivers, points):
    row_span = receivers // block_map.shape[0]
    col_span = points // block_map.shape[1]
    return jnp.repeat(jnp.repeat(block_map, row_span, axis=0), col_span, axis=1).astype(
        jnp.bfloat16
    )


def transform(cos_table, records, length):
    spectrum = jnp.dot(cos_table, records.reshape(length, -1), preferred_element_type=jnp.float32)
    return (spectrum * (1.0 / math.sqrt(length))).astype(jnp.bfloat16)


def back_project(spectra, masked):
    swapped = jnp.stack((spectra[:, 1], -spectra[:, 0]), axis=1)
    blocks = jnp.stack((spectra, swapped), axis=1)
    return jnp.einsum("fcrx,focrs->fosx", masked, blocks, preferred_element_type=jnp.float32)


def body(traces, freq_index, block_map, green_rec, green_src):
    shards = lax.axis_size("freq")
    length = traces.shape[0] * shards
    receivers = traces.shape[1]
    shots = traces.shape[2]
    freqs = freq_index.shape[0]
    cos_table = dft_table(freq_index, length)
    masked = green_rec * expand_map(block_map, receivers, green_rec.shape[3])[None, None]
    regrouped = lax.all_to_all(traces, "freq", split_axis=2, concat_axis=0, tiled=True)
    spectrum = transform(cos_table, regrouped, length).reshape(freqs, 2, receivers, shots // shards)
    gathered = lax.all_to_all(spectrum, "freq", split_axis=0, concat_axis=3, tiled=True)
    back_field = back_project(gathered, masked)
    partial_image = jnp.sum(green_src.astype(jnp.float32) * back_field, axis=(0, 1, 2))
    return lax.psum_scatter(partial_image, "freq", scatter_dimension=0, tiled=True)


CORES = 2
ROWS = 2
LAG = 4
LANES = 128


def bands(half):
    return tuple((start, LANES) for start in range(0, half, LANES))


def seat(cols, row, core):
    return (cols * ROWS + row) * CORES + core


def remote(src, dst, send_sem, recv_sem, target):
    return pltpu.make_async_remote_copy(
        src_ref=src,
        dst_ref=dst,
        send_sem=send_sem,
        recv_sem=recv_sem,
        device_id={"freq": target},
        device_id_type=pl.DeviceIdType.MESH,
    )


def imaging_kernel(
    shots,
    x_ref,
    fi_hbm,
    map_ref,
    green_ref,
    src_ref,
    out_ref,
    fi_ref,
    x_all,
    x_far,
    table,
    y_send,
    y_own,
    y_recv,
    z_send,
    z_own,
    z_recv,
    green_v,
    src_v,
    map_v,
    mask_v,
    acc,
    i_send,
    i_recv,
    x_sem,
    load_sem,
    far_send,
    far_recv,
    ys_sem,
    yr_sem,
    zs_sem,
    zr_sem,
    is_sem,
    ir_sem,
    up_sem,
    down_sem,
    pair_sem,
    row_sem,
):
    shards = i_send.shape[0]
    cols = shards // (ROWS * CORES)
    local_rows, half = x_far.shape
    samples = local_rows // shots
    length = samples * shards
    band = y_own.shape[0]
    steps = bands(half)
    chunks = len(steps)
    freqs = fi_ref.shape[0]
    receivers = CORES * half
    points = acc.shape[1]
    block = 2 * shots
    bf16, f32 = jnp.bfloat16, jnp.float32

    me = lax.axis_index("freq")
    core = lax.rem(me, CORES)
    row = lax.rem(me // CORES, ROWS)
    col = me // (CORES * ROWS)
    mate = seat(col, row, 1 - core)
    across = seat(col, 1 - row, core)

    barrier = pltpu.get_barrier_semaphore()

    def tell(sem, target):
        pl.semaphore_signal(
            sem, inc=1, device_id={"freq": target}, device_id_type=pl.DeviceIdType.MESH
        )

    tell(barrier, mate)
    tell(barrier, across)

    @pl.when(col > 0)
    def _():
        tell(barrier, seat(col - 1, row, core))

    @pl.when(col < cols - 1)
    def _():
        tell(barrier, seat(col + 1, row, core))

    def relay(hop):
        @pl.when(col == hop)
        def _():
            if hop > 0:
                pl.semaphore_wait(up_sem, 1)
            if hop < cols - 1:
                tell(up_sem, seat(col + 1, row, core))

        @pl.when(col == cols - 1 - hop)
        def _():
            if hop > 0:
                pl.semaphore_wait(down_sem, 1)
            if hop < cols - 1:
                tell(down_sem, seat(col - 1, row, core))

    def lanes(core_at, k):
        return pl.ds(pl.multiple_of(core_at * half + steps[k][0], LANES), steps[k][1])

    def x_load(core_at):
        side = pl.ds(pl.multiple_of(core_at * half, LANES), half)
        return pltpu.make_async_copy(x_ref.at[:, side], x_all.at[:, side], x_sem.at[core_at])

    def far_copy(k):
        return remote(
            x_all.at[:, lanes(1 - core, k)],
            x_far.at[:, pl.ds(*steps[k])],
            far_send,
            far_recv.at[k],
            mate,
        )

    fi_load = pltpu.make_async_copy(fi_hbm, fi_ref, load_sem.at[3])
    map_load = pltpu.make_async_copy(map_ref, map_v, load_sem.at[0])
    src_load = pltpu.make_async_copy(src_ref, src_v, load_sem.at[1])
    green_load = pltpu.make_async_copy(green_ref, green_v, load_sem.at[2])
    fi_load.start()
    x_load(1 - core).start()
    x_load(core).start()
    map_load.start()
    src_load.start()
    green_load.start()

    table_rows = 2 * freqs
    span = CORES * samples
    line = lax.broadcasted_iota(jnp.int32, (table_rows, span), 0)
    column = lax.broadcasted_iota(jnp.int32, (table_rows, span), 1)
    fi_load.wait()
    bins = jnp.zeros((table_rows, span), jnp.int32)
    for f in range(freqs):
        place = ((f // CORES) % ROWS * cols + f // (CORES * ROWS)) * CORES + f % CORES
        bins = jnp.where(line // 2 == place, fi_ref[f], bins)
    time = jnp.where(column < samples, me * samples + column, (mate - 1) * samples + column)
    angles = lax.rem(bins * time, length).astype(f32) * f32(2.0 * math.pi / length)
    small = jnp.where(line % 2 == 0, jnp.cos(angles), -jnp.sin(angles)).astype(bf16)
    wide = span * shots
    spread = lax.broadcasted_iota(jnp.int32, (span, wide), 1) // shots == lax.broadcasted_iota(
        jnp.int32, (span, wide), 0
    )
    stretched = jnp.dot(small, jnp.where(spread, 1.0, 0.0).astype(bf16), preferred_element_type=f32)
    same_shot = lax.broadcasted_iota(jnp.int32, (shots, wide), 1) % shots == lax.broadcasted_iota(
        jnp.int32, (shots, wide), 0
    )
    for r in range(table_rows):
        spread_row = jnp.broadcast_to(stretched[r : r + 1, :], (shots, wide))
        table[r * shots : (r + 1) * shots, :] = jnp.where(same_shot, spread_row, 0.0).astype(bf16)

    greeted = 2 + jnp.minimum(col, 1) + jnp.minimum(cols - 1 - col, 1)
    pl.semaphore_wait(barrier, greeted)
    x_load(1 - core).wait()
    for k in range(chunks):
        far_copy(k).start()

    def partial(side, k):
        rows = pl.ds(pl.multiple_of(side * band, band), band)
        at = pl.ds(*steps[k])
        near = jnp.dot(table[rows, :local_rows], x_all[:, lanes(core, k)], preferred_element_type=f32)
        return near + jnp.dot(table[rows, local_rows:], x_far[:, at], preferred_element_type=f32)

    def y_copy(k):
        at = pl.ds(*steps[k])
        return remote(y_send.at[:, at], y_recv.at[:, at], ys_sem, yr_sem.at[k], across)

    def send_partial(k):
        far_copy(k).wait_recv()
        y_send[:, pl.ds(*steps[k])] = partial(1 - row, k).astype(bf16)
        y_copy(k).start()

    def keep_partial(k):
        y_own[:, pl.ds(*steps[k])] = partial(row, k)

    def block_rows(col_at, core_at):
        return pl.ds(pl.multiple_of((col_at * CORES + core_at) * block, block), block)

    peers = [(dc, dk) for dc in range(cols) for dk in range(CORES) if dc or dk]

    def z_copy(k, dc, dk):
        to_col = lax.rem(col + dc, cols)
        to_core = lax.rem(core + dk, CORES)
        return remote(
            z_send.at[block_rows(to_col, to_core), pl.ds(*steps[k])],
            z_recv.at[col, :, lanes(core, k)],
            zs_sem,
            zr_sem.at[k],
            seat(to_col, row, to_core),
        )

    def scatter(k):
        y_copy(k).wait_recv()
        at = pl.ds(*steps[k])
        y_own[:, at] = y_own[:, at] + y_recv[:, at].astype(f32)
        z_send[:, at] = y_own[:, at].astype(bf16)
        for dc, dk in peers:
            z_copy(k, dc, dk).start()
        z_own[:, at] = y_own[block_rows(col, core), at]
    x_load(core).wait()
    relay(0)
    for k in range(chunks):
        send_partial(k)
        if k % 2 == 1 and (k + 1) // 2 < cols:
            relay((k + 1) // 2)
        if k % 4 == 3:
            keep_partial(k // 4)
    early = (chunks + 3) // 4
    for k in range(chunks // 4, early):
        keep_partial(k)
    for hop in range(chunks // 2 + 1, cols):
        relay(hop)
    tell(pair_sem, mate)
    pl.semaphore_wait(pair_sem, 1)
    tell(row_sem, across)
    scatter(0)
    keep_partial(early)
    scatter(1)
    for k in range(early + 1, min(early + 2, chunks)):
        keep_partial(k)

    map_load.wait()
    tiles = map_v.shape[1]
    in_tile = lax.broadcasted_iota(jnp.int32, (tiles, points), 1) // (
        points // tiles
    ) == lax.broadcasted_iota(jnp.int32, (tiles, points), 0)
    mask_v[...] = jnp.dot(
        map_v[...].astype(f32).astype(bf16),
        jnp.where(in_tile, 1.0, 0.0).astype(bf16),
        preferred_element_type=f32,
    )
    green_load.wait()
    deep = receivers // map_v.shape[0]

    def mask_block(i, carry):
        seen = jnp.broadcast_to(mask_v[pl.ds(i, 1), :], (deep, points)).astype(bf16)
        for part in range(2):
            at = pl.ds(pl.multiple_of(part * receivers + i * deep, deep), deep)
            green_v[at, :] = green_v[at, :] * seen
        return carry

    lax.fori_loop(0, map_v.shape[0], mask_block, 0)
    acc[...] = jnp.zeros_like(acc)

    def z_arrival(k):
        every = z_send.at[pl.ds(0, len(peers) * block), pl.ds(*steps[k])]
        return pltpu.make_async_copy(every, every, zr_sem.at[k])

    def use(spectrum, core_at, k):
        spectrum = spectrum * f32(1.0 / math.sqrt(length))
        turned = jnp.concatenate((spectrum[shots:], -spectrum[:shots]), axis=0)
        first = lanes(core_at, k)
        second = lanes(CORES + core_at, k)
        acc[...] += jnp.dot(
            spectrum.astype(bf16), green_v[first, :], preferred_element_type=f32
        ) + jnp.dot(turned.astype(bf16), green_v[second, :], preferred_element_type=f32)

    def consume(k):
        z_arrival(k).wait()
        for dk in range(CORES):
            from_core = lax.rem(core + dk, CORES)
            total = None if dk else z_own[:, pl.ds(*steps[k])]
            for dc in range(cols):
                if dc or dk:
                    from_col = lax.rem(col + cols - dc, cols)
                    term = z_recv[from_col, :, lanes(from_core, k)].astype(f32)
                    total = term if total is None else total + term
            use(total, from_core, k)

    for k in range(2, chunks):
        scatter(k)
        for at in range(early + 2 * k - 2, min(early + 2 * k, chunks)):
            keep_partial(at)
        if k >= LAG:
            consume(k - LAG)
    for k in range(chunks - LAG, chunks):
        consume(k)

    src_load.wait()
    product = src_v[...].astype(f32) * acc[...]
    folded = product[0:8]
    for at in range(8, block, 8):
        folded = folded + product[at : at + 8]
    flat = jnp.broadcast_to(jnp.sum(folded, axis=0, keepdims=True), (8, points))
    each = points // shards
    for d in range(shards):
        i_send[d] = pltpu.roll(flat, (points - d * each) % points, 1)[0:1, :LANES]

    def i_copy(step):
        to = lax.rem(me + step, shards)
        return remote(i_send.at[to], i_recv.at[step], is_sem, ir_sem, to)

    pl.semaphore_wait(row_sem, 1)
    for step in range(1, shards):
        i_copy(step).start()
    total = i_send[me]
    others = i_recv.at[pl.ds(1, shards - 1)]
    pltpu.make_async_copy(others, others, ir_sem).wait()
    for step in range(1, shards):
        total = total + i_recv[step]
    out_ref[...] = total

    z_sent = z_send.at[pl.ds(0, len(peers) * block), :]
    for sent, sem in ((x_far, far_send), (y_send, ys_sem), (z_sent, zs_sem), (others, is_sem)):
        pltpu.make_async_copy(sent, sent, sem).wait()


def fused_body(traces, freq_index, block_map, green_rec, green_src):
    shards = lax.axis_size("freq")
    samples, receivers, shots = traces.shape
    points = green_rec.shape[3]
    freqs = freq_index.shape[0]
    cols = shards // (ROWS * CORES)
    half = receivers // CORES
    chunks = len(bands(half))
    records = jnp.transpose(traces, (0, 2, 1)).reshape(samples * shots, receivers)
    green = green_rec.reshape(2 * receivers, points)
    sources = green_src.reshape(2 * shots, points)
    band = 2 * freqs * shots // ROWS
    block = 2 * shots
    bf16, f32 = jnp.bfloat16, jnp.float32
    dma = pltpu.SemaphoreType.DMA
    outside = pl.BlockSpec(memory_space=pltpu.HBM)
    image = pl.pallas_call(
        functools.partial(imaging_kernel, shots),
        out_shape=jax.ShapeDtypeStruct((1, LANES), f32),
        in_specs=[outside] * 5,
        out_specs=pl.BlockSpec(memory_space=pltpu.VMEM),
        scratch_shapes=[
            pltpu.SMEM(freq_index.shape, jnp.int32),
            pltpu.VMEM((samples * shots, receivers), bf16),
            pltpu.VMEM((samples * shots, half), bf16),
            pltpu.VMEM((2 * freqs * shots, CORES * samples * shots), bf16),
            pltpu.VMEM((band, half), bf16),
            pltpu.VMEM((band, half), f32),
            pltpu.VMEM((band, half), bf16),
            pltpu.VMEM((band, half), bf16),
            pltpu.VMEM((block, half), f32),
            pltpu.VMEM((cols, block, receivers), bf16),
            pltpu.VMEM((2 * receivers, points), bf16),
            pltpu.VMEM((block, points), bf16),
            pltpu.VMEM(block_map.shape, jnp.int32),
            pltpu.VMEM((block_map.shape[0], points), f32),
            pltpu.VMEM((block, points), f32),
            pltpu.VMEM((shards, 1, LANES), f32),
            pltpu.VMEM((shards, 1, LANES), f32),
            dma((CORES,)),
            dma((4,)),
            dma,
            dma((chunks,)),
            dma,
            dma((chunks,)),
            dma,
            dma((chunks,)),
            dma,
            dma,
        ]
        + [pltpu.SemaphoreType.REGULAR] * 4,
        compiler_params=pltpu.CompilerParams(
            collective_id=0, has_side_effects=True, vmem_limit_bytes=48 * 1024 * 1024
        ),
    )(
        *(
            pltpu.with_memory_space_constraint(array, pltpu.HBM)
            for array in (records, freq_index, block_map, green, sources)
        )
    )
    return image[0, : points // shards]


def moves_less(traces, freq_index, green_rec):
    shards = lax.axis_size("freq")
    samples, receivers, shots = traces.shape
    freqs = freq_index.shape[0]
    return (
        2 * freqs <= samples
        and freqs == shards
        and shards % (ROWS * CORES) == 0
        and shots % 16 == 0
        and receivers % (CORES * 4 * LANES) == 0
        and green_rec.shape[3] % LANES == 0
        and green_rec.shape[3] // shards <= LANES
    )


def chosen_body(traces, freq_index, block_map, green_rec, green_src):
    fused = moves_less(traces, freq_index, green_rec)
    return (fused_body if fused else body)(traces, freq_index, block_map, green_rec, green_src)


def solution(mesh):
    in_specs = (
        P("freq", None, "groups"),
        P(),
        P(),
        P("freq", None, None, "groups"),
        P("freq", None, None, "groups"),
    )
    out_specs = P(("groups", "freq"))
    return jax.shard_map(chosen_body, mesh=mesh, in_specs=in_specs, out_specs=out_specs, check_vma=False)
```
